32 devices in a mesh: rep: 1 (over z), tp: 4 (over y), sp: 8 (over x, core).
Axes of the slice: x: 4, y: 4, z: 1, core: 2. Of those that a mesh axis runs over, the one named last changes fastest.
The devices are a block of a 4x4x8 slice.
Arguments:
- x_in: bfloat16 [4096, 5120], P(('rep', 'sp'))
- positions: int32 [4096], P(('rep', 'sp'))
- norm_gain: float32 [5120], replicated
- w_q: bfloat16 [5120, 4096], P(None, 'tp')
- w_k: bfloat16 [5120, 1024], P(None, 'tp')
- w_v: bfloat16 [5120, 1024], P(None, 'tp')
- w_o: bfloat16 [4096, 5120], P('tp')
- w_gate: bfloat16 [5120, 32768], P(None, 'tp')
- w_up: bfloat16 [5120, 32768], P(None, 'tp')
- w_down: bfloat16 [32768, 5120], P('tp')
Outputs:
- output 1: bfloat16 [4096, 5120], P(('rep', 'sp'))
- output 2: bfloat16 [4096, 32, 128], P('rep', ('tp', 'sp'))
- output 3: bfloat16 [4096, 32, 128], P('rep', ('tp', 'sp'))
All inputs are finite; a program needn't handle non-finite values.
Results may differ from the reference program's by a relative error of at most 0.00236406.
Values are sent between devices in bfloat16 or wider.
A program may use at most 768 MiB of HBM per device.

```python
import math
import jax
import jax.numpy as jnp
from jax import lax

MODEL_DIM = 5120
NUM_HEADS = 32
KV_HEADS = 8
HEAD_DIM = 128
FF_DIM = 32768
TOKENS = 4096
GROUP_DEVS = 32
DOC_COUNT = 8

KV_REPEAT = max(GROUP_DEVS // KV_HEADS, 1)
GROUP_SIZE = NUM_HEADS // KV_HEADS
ROW_BLOCK = min(TOKENS, 64)
NUM_BLOCKS = TOKENS // ROW_BLOCK
EPS = 1e-6
ROPE_BASE = 500000.0
SCORE_SCALE = 1.0 / math.sqrt(HEAD_DIM)


def setup_inputs(seed: int = 0, part: int = 0) -> dict:
    part_keys = jax.random.split(jax.random.fold_in(jax.random.key(seed), part), 3)
    shared_keys = jax.random.split(jax.random.key(seed + 1), 8)

    def weight(key_w, fan_in, fan_out):
        return (jax.random.normal(key_w, (fan_in, fan_out), jnp.float32) * fan_in ** -0.5).astype(jnp.bfloat16)

    noise_part = jax.random.normal(part_keys[0], (DOC_COUNT, TOKENS // DOC_COUNT, MODEL_DIM), jnp.float32)
    doc_means = jax.random.normal(part_keys[1], (DOC_COUNT, 1, MODEL_DIM), jnp.float32)
    x_in = (noise_part + doc_means).reshape(TOKENS, MODEL_DIM).astype(jnp.bfloat16)
    start_pos = jax.random.randint(part_keys[2], (), 0, TOKENS)
    positions = (start_pos + jnp.arange(TOKENS)).astype(jnp.int32)
    norm_gain = 1.0 + 0.3 * jax.random.normal(shared_keys[0], (MODEL_DIM,), jnp.float32)
    return {
        "x_in": x_in,
        "positions": positions,
        "norm_gain": norm_gain,
        "w_q": weight(shared_keys[1], MODEL_DIM, NUM_HEADS * HEAD_DIM),
        "w_k": weight(shared_keys[2], MODEL_DIM, KV_HEADS * HEAD_DIM),
        "w_v": weight(shared_keys[3], MODEL_DIM, KV_HEADS * HEAD_DIM),
        "w_o": weight(shared_keys[4], NUM_HEADS * HEAD_DIM, MODEL_DIM),
        "w_gate": weight(shared_keys[5], MODEL_DIM, FF_DIM),
        "w_up": weight(shared_keys[6], MODEL_DIM, FF_DIM),
        "w_down": weight(shared_keys[7], FF_DIM, MODEL_DIM),
    }


def rotate(vectors, cos_tab, sin_tab):
    half_dim = HEAD_DIM // 2
    lower_part = vectors[..., :half_dim]
    upper_part = vectors[..., half_dim:]
    return jnp.concatenate([lower_part * cos_tab - upper_part * sin_tab, upper_part * cos_tab + lower_part * sin_tab], axis=-1).astype(jnp.bfloat16)


def reference(x_in, positions, norm_gain, w_q, w_k, w_v, w_o, w_gate, w_up, w_down):
    x_f32 = x_in.astype(jnp.float32)
    inv_rms = lax.rsqrt(jnp.mean(x_f32 * x_f32, axis=-1, keepdims=True) + EPS)
    normed = (x_f32 * inv_rms * norm_gain).astype(jnp.bfloat16)
    inv_freq = ROPE_BASE ** (-(jnp.arange(HEAD_DIM // 2, dtype=jnp.float32) * (2.0 / HEAD_DIM)))
    angles = positions.astype(jnp.float32)[:, None] * inv_freq[None, :]
    cos_tab = jnp.cos(angles)[:, None, :]
    sin_tab = jnp.sin(angles)[:, None, :]
    q_rot = rotate(jnp.dot(normed, w_q, preferred_element_type=jnp.float32).reshape(TOKENS, NUM_HEADS, HEAD_DIM), cos_tab, sin_tab)
    k_rot = rotate(jnp.dot(normed, w_k, preferred_element_type=jnp.float32).reshape(TOKENS, KV_HEADS, HEAD_DIM), cos_tab, sin_tab)
    v_val = jnp.dot(normed, w_v, preferred_element_type=jnp.float32).astype(jnp.bfloat16).reshape(TOKENS, KV_HEADS, HEAD_DIM)
    q_grouped = q_rot.reshape(TOKENS, KV_HEADS, GROUP_SIZE, HEAD_DIM).astype(jnp.float32)
    k_f32 = k_rot.astype(jnp.float32)
    v_f32 = v_val.astype(jnp.float32)
    key_idx = jnp.arange(TOKENS)

    def attend_block(block_id):
        q_tile = lax.dynamic_slice_in_dim(q_grouped, block_id * ROW_BLOCK, ROW_BLOCK, axis=0)
        scores = jnp.einsum("qcgd,kcd->cgqk", q_tile, k_f32) * SCORE_SCALE
        query_idx = block_id * ROW_BLOCK + jnp.arange(ROW_BLOCK)
        scores = jnp.where(key_idx[None, :] <= query_idx[:, None], scores, -jnp.inf)
        weights = jnp.exp(scores - jnp.max(scores, axis=-1, keepdims=True))
        weight_total = jnp.sum(weights, axis=-1)
        weighted_sum = jnp.einsum("cgqk,kcd->qcgd", weights.astype(jnp.bfloat16).astype(jnp.float32), v_f32)
        return (weighted_sum / jnp.transpose(weight_total, (2, 0, 1))[..., None]).astype(jnp.bfloat16)

    attn_out = lax.map(attend_block, jnp.arange(NUM_BLOCKS)).reshape(TOKENS, NUM_HEADS * HEAD_DIM)
    attn_proj = jnp.dot(attn_out, w_o, preferred_element_type=jnp.float32)
    gate_acc = jnp.dot(normed, w_gate, preferred_element_type=jnp.float32)
    up_acc = jnp.dot(normed, w_up, preferred_element_type=jnp.float32)
    hidden = (jax.nn.silu(gate_acc) * up_acc).astype(jnp.bfloat16)
    mlp_out = jnp.dot(hidden, w_down, preferred_element_type=jnp.float32)
    y_out = (x_f32 + attn_proj + mlp_out).astype(jnp.bfloat16)
    k_cache = jnp.repeat(k_rot, KV_REPEAT, axis=1)
    v_cache = jnp.repeat(v_val, KV_REPEAT, axis=1)
    return y_out, k_cache, v_cache
```

```python
import functools

import jax
import jax.numpy as jnp
from jax import lax
from jax.experimental import pallas as pl
from jax.experimental.pallas import tpu as pltpu
from jax.sharding import PartitionSpec as P

HEAD_DIM = 128
EPS = 1e-6
ROPE_BASE = 500000.0
SCORE_SCALE = HEAD_DIM ** -0.5
F32 = jnp.float32
BF16 = jnp.bfloat16
MESH = pl.DeviceIdType.MESH
VMEM_LIMIT = 66 * 1000 * 1000

GW = 256
NW = 2 * GW
TW = 256
HW = TW // 2
SLOTS = 3
LAG = 2


def rms_norm(x_in, norm_gain):
    x_f32 = x_in.astype(F32)
    inv_rms = lax.rsqrt(jnp.mean(x_f32 * x_f32, axis=-1, keepdims=True) + EPS)
    return (x_f32 * inv_rms * norm_gain).astype(BF16)


def rope_tables(positions):
    inv_freq = ROPE_BASE ** (-(jnp.arange(HEAD_DIM // 2, dtype=F32) * (2.0 / HEAD_DIM)))
    angles = positions.astype(F32)[:, None] * inv_freq[None, :]
    return jnp.cos(angles)[:, None, :], jnp.sin(angles)[:, None, :]


def rotate(vectors, cos_tab, sin_tab):
    half_dim = HEAD_DIM // 2
    lower_part = vectors[..., :half_dim]
    upper_part = vectors[..., half_dim:]
    return jnp.concatenate([lower_part * cos_tab - upper_part * sin_tab, upper_part * cos_tab + lower_part * sin_tab], axis=-1).astype(BF16)


def attention_kernel(q_ref, k_ref, v_ref, o_ref, s_ref, *, rows):
    tile = pl.program_id(0)

    def score(block, masked):
        keys = k_ref[pl.ds(block * rows, rows), :]
        s = lax.dot_general(q_ref[...], keys, (((1,), (1,)), ((), ())), preferred_element_type=F32)
        if masked:
            row = lax.broadcasted_iota(jnp.int32, (rows, rows), 0)
            col = lax.broadcasted_iota(jnp.int32, (rows, rows), 1)
            s = jnp.where(col <= row, s, -jnp.inf)
        s_ref[block] = s
        top = s[:, :128]
        for g in range(1, rows // 128):
            top = jnp.maximum(top, s[:, g * 128:(g + 1) * 128])
        return top

    top = score(tile, True)
    top = lax.fori_loop(0, tile, lambda b, t: jnp.maximum(t, score(b, False)), top)
    row_max = jnp.max(top, axis=-1, keepdims=True) * SCORE_SCALE

    def gather(block, carry):
        total, acc = carry
        p = jnp.exp(s_ref[block] * SCORE_SCALE - row_max)
        for g in range(rows // 128):
            total = total + p[:, g * 128:(g + 1) * 128]
        acc = acc + jnp.dot(p.astype(BF16), v_ref[pl.ds(block * rows, rows), :], preferred_element_type=F32)
        return total, acc

    zero = jnp.zeros((rows, HEAD_DIM), F32)
    total, acc = lax.fori_loop(0, tile + 1, gather, (zero, zero))
    o_ref[...] = (acc / jnp.sum(total, axis=-1, keepdims=True)).astype(BF16)


def attention(q_all, k_all, v_all):
    tokens = q_all.shape[0]
    rows = min(512, tokens)
    tiles = tokens // rows
    whole = pl.BlockSpec((tokens, HEAD_DIM), lambda t: (0, 0))
    part = pl.BlockSpec((rows, HEAD_DIM), lambda t: (t, 0))
    return pl.pallas_call(
        functools.partial(attention_kernel, rows=rows),
        grid=(tiles,),
        out_shape=jax.ShapeDtypeStruct((tokens, HEAD_DIM), BF16),
        in_specs=[part, whole, whole],
        out_specs=part,
        scratch_shapes=[pltpu.VMEM((tiles, rows, rows), F32)],
        compiler_params=pltpu.CompilerParams(vmem_limit_bytes=48 * 1000 * 1000),
        cost_estimate=pl.CostEstimate(flops=2 * tokens * tokens * HEAD_DIM, bytes_accessed=8 * tokens * HEAD_DIM, transcendentals=tokens * tokens // 2),
    )(q_all, k_all, v_all)


def ring_kernel(
    ring,
    u_hbm, x_hbm, attn_hbm, wo_hbm, wg_hbm, wu_hbm, wd_hbm,
    y_hbm,
    slots, u, attn, xown, hid, part, far, near, ybuf,
    w_sem, ld_sem, far_sem, near_sem, ag_sem, fw_sem, send_sem, out_sem,
):
    tokens, width = u.shape
    ff = hid.shape[1]
    heads = attn.shape[1]
    rows = tokens // 2
    own = rows // ring
    gu_steps = ff // GW
    dn_tiles = width // NW
    chunk_steps = gu_steps + 2 * dn_tiles
    depth = (ff + heads) // 2
    tiles = width // TW
    all_tiles = 2 * tiles

    me = lax.axis_index("tp")
    right = lax.rem(me + 1, ring)
    left = lax.rem(me + ring - 1, ring)
    opp = lax.rem(me + 2, ring)

    def block_rows(owner):
        return pl.ds(pl.multiple_of(owner * own, own), own)

    def local(src, dst, sem):
        return pltpu.make_async_copy(src, dst, sem)

    def remote(src, dst, send, recv, who):
        return pltpu.make_async_remote_copy(src_ref=src, dst_ref=dst, send_sem=send, recv_sem=recv, device_id={"tp": who}, device_id_type=MESH)


    def issue(step):
        r = lax.rem(step, chunk_steps)
        slot = lax.rem(step, SLOTS)
        live = step < 2 * chunk_steps
        q = r - gu_steps
        tile_cols = pl.ds(pl.multiple_of(lax.div(jnp.maximum(q, 0), 2) * NW, NW), NW)

        @pl.when(jnp.logical_and(live, r < gu_steps))
        def _():
            cols = pl.ds(pl.multiple_of(r * GW, GW), GW)
            local(wg_hbm.at[:, cols], slots.at[slot, 0:width, 0:GW], w_sem.at[slot]).start()
            local(wu_hbm.at[:, cols], slots.at[slot, 0:width, GW:NW], w_sem.at[slot]).start()

        @pl.when(jnp.logical_and(live, jnp.logical_and(q >= 0, lax.rem(q, 2) == 0)))
        def _():
            local(wd_hbm.at[0:depth, tile_cols], slots.at[slot, 0:depth, :], w_sem.at[slot]).start()

        @pl.when(jnp.logical_and(live, jnp.logical_and(q >= 0, lax.rem(q, 2) == 1)))
        def _():
            local(wd_hbm.at[depth:ff, tile_cols], slots.at[slot, 0:ff - depth, :], w_sem.at[slot]).start()
            local(wo_hbm.at[:, tile_cols], slots.at[slot, ff - depth:depth, :], w_sem.at[slot]).start()

    def arrived(step, deep):
        slot = lax.rem(step, SLOTS)
        local(wd_hbm.at[0:deep, 0:NW], slots.at[slot, 0:deep, :], w_sem.at[slot]).wait()
        return slot


    def tick_pre(k):
        @pl.when(jnp.logical_and(k >= LAG, k < all_tiles + LAG))
        def _():
            t = k - LAG
            local(far.at[t], far.at[t], far_sem.at[t]).wait()
            part[t, block_rows(left), 0:HW] += far[t, 0]
            part[t, block_rows(right), HW:TW] += far[t, 1]

        @pl.when(jnp.logical_and(k >= 2 * LAG, k < all_tiles + 2 * LAG))
        def _():
            t = k - 2 * LAG
            local(near.at[t], near.at[t], near_sem.at[t]).wait()
            chunk = lax.div(t, tiles)
            cols = pl.ds(pl.multiple_of(lax.rem(t, tiles) * TW, TW), TW)
            total = (part[t, block_rows(me), :] + near[t, 0]) + near[t, 1]
            ybuf[t, block_rows(me), :] = (xown[chunk, :, cols].astype(F32) + total).astype(BF16)

    def tick_post(k):
        @pl.when(jnp.logical_and(k >= 3 * LAG, k < all_tiles + 3 * LAG))
        def _():
            t = k - 3 * LAG
            local(ybuf.at[t, 0:2 * own], ybuf.at[t, 0:2 * own], ag_sem.at[t]).wait()
            here = ybuf.at[t, block_rows(right), 0:HW]
            remote(here, here, send_sem.at[3], fw_sem.at[t], left).start()
            here = ybuf.at[t, block_rows(left), HW:TW]
            remote(here, here, send_sem.at[3], fw_sem.at[t], right).start()

        @pl.when(jnp.logical_and(k >= 2 * LAG, k < all_tiles + 2 * LAG))
        def _():
            t = k - 2 * LAG
            here = ybuf.at[t, block_rows(me), :]
            remote(here, here, send_sem.at[2], ag_sem.at[t], left).start()
            remote(here, here, send_sem.at[2], ag_sem.at[t], right).start()

        @pl.when(jnp.logical_and(k >= LAG, k < all_tiles + LAG))
        def _():
            t = k - LAG
            remote(part.at[t, block_rows(left), 0:HW], near.at[t, 0, :, 0:HW], send_sem.at[1], near_sem.at[t], left).start()
            remote(part.at[t, block_rows(right), HW:TW], near.at[t, 1, :, HW:TW], send_sem.at[1], near_sem.at[t], right).start()

        @pl.when(k < all_tiles)
        def _():
            t = k
            remote(part.at[t, block_rows(opp), 0:HW], far.at[t, 0], send_sem.at[0], far_sem.at[t], left).start()
            remote(part.at[t, block_rows(opp), HW:TW], far.at[t, 1], send_sem.at[0], far_sem.at[t], right).start()
            remote(part.at[t, block_rows(left), HW:TW], near.at[t, 0, :, HW:TW], send_sem.at[0], near_sem.at[t], left).start()
            remote(part.at[t, block_rows(right), 0:HW], near.at[t, 1, :, 0:HW], send_sem.at[0], near_sem.at[t], right).start()

        @pl.when(k >= 4 * LAG)
        def _():
            t = k - 4 * LAG
            local(ybuf.at[t, 0:own], ybuf.at[t, 0:own], fw_sem.at[t]).wait()
            there = y_hbm.at[pl.ds(pl.multiple_of(lax.div(t, tiles) * rows, rows), rows), pl.ds(pl.multiple_of(lax.rem(t, tiles) * TW, TW), TW)]
            local(ybuf.at[t], there, out_sem).start()


    for step in range(SLOTS - 1):
        issue(jnp.int32(step))
    loads = [local(u_hbm, u, ld_sem.at[0]), local(attn_hbm, attn, ld_sem.at[1])]
    for chunk in range(2):
        mine = pl.ds(pl.multiple_of(chunk * rows + me * own, own), own)
        loads.append(local(x_hbm.at[mine, :], xown.at[chunk], ld_sem.at[2 + chunk]))
    for load in loads:
        load.start()

    barrier = pltpu.get_barrier_semaphore()
    for neighbour in (left, right):
        pl.semaphore_signal(barrier, inc=1, device_id={"tp": neighbour}, device_id_type=MESH)
    pl.semaphore_wait(barrier, 2)
    for load in loads:
        load.wait()

    gu_ticks = tiles - dn_tiles
    period = gu_steps // gu_ticks

    def chunk_body(chunk, carry):
        base = chunk * chunk_steps
        row0 = pl.multiple_of(chunk * rows, rows)

        def gu_body(j, c):
            step = base + j
            ticks = jnp.logical_and(jnp.logical_and(chunk == 1, lax.rem(j, period) == period - 1), lax.div(j, period) < gu_ticks)
            k = dn_tiles - 1 + lax.div(j, period)

            @pl.when(ticks)
            def _():
                tick_pre(k)

            issue(step + SLOTS - 1)
            slot = arrived(step, width)
            both = jnp.dot(u[pl.ds(row0, rows), :], slots[slot, 0:width, :], preferred_element_type=F32)
            gate = both[:, :GW]
            act = (gate * jax.nn.sigmoid(gate)) * both[:, GW:]
            hid[:, pl.ds(pl.multiple_of(j * GW, GW), GW)] = act.astype(BF16)

            @pl.when(ticks)
            def _():
                tick_post(k)

            return c

        lax.fori_loop(0, gu_steps, gu_body, 0)

        def dn_body(j, c):
            step = base + gu_steps + 2 * j
            k = chunk * tiles + j - 1
            t = chunk * tiles + 2 * j

            @pl.when(k >= 0)
            def _():
                tick_pre(k)

            issue(step + SLOTS - 1)
            slot = arrived(step, depth)
            first = jnp.dot(hid[:, 0:depth], slots[slot, 0:depth, :], preferred_element_type=F32)
            for half in range(NW // TW):
                part[t + half] = first[:, half * TW:(half + 1) * TW]

            @pl.when(k >= 0)
            def _():
                tick_post(k)

            issue(step + SLOTS)
            slot = arrived(step + 1, depth)
            second = jnp.dot(hid[:, depth:ff], slots[slot, 0:ff - depth, :], preferred_element_type=F32)
            second = second + jnp.dot(attn[pl.ds(row0, rows), :], slots[slot, ff - depth:depth, :], preferred_element_type=F32)
            for half in range(NW // TW):
                part[t + half] += second[:, half * TW:(half + 1) * TW]
            return c

        lax.fori_loop(0, dn_tiles, dn_body, 0)
        return carry

    lax.fori_loop(0, 2, chunk_body, 0)

    def tail_body(k, c):
        tick_pre(k)
        tick_post(k)
        return c

    lax.fori_loop(tiles + dn_tiles - 1, all_tiles + 4 * LAG, tail_body, 0)

    local(part.at[0:tiles], part.at[0:tiles], send_sem.at[0]).wait()
    local(far, far, send_sem.at[1]).wait()
    local(ybuf.at[0:tiles], ybuf.at[0:tiles], send_sem.at[2]).wait()
    local(ybuf.at[0:tiles // 2], ybuf.at[0:tiles // 2], send_sem.at[3]).wait()
    local(ybuf, ybuf, out_sem).wait()


def ring_mlp(ring, normed, x_in, attn_tok, w_o, w_gate, w_up, w_down):
    tokens, width = x_in.shape
    ff = w_down.shape[0]
    heads = w_o.shape[0]
    rows = tokens // 2
    own = rows // ring
    all_tiles = 2 * (width // TW)
    depth = (ff + heads) // 2
    anywhere = pl.BlockSpec(memory_space=pl.ANY)
    flops = 2 * tokens * width * (3 * ff + heads)
    return pl.pallas_call(
        functools.partial(ring_kernel, ring),
        out_shape=jax.ShapeDtypeStruct((tokens, width), BF16),
        in_specs=[anywhere] * 7,
        out_specs=anywhere,
        scratch_shapes=[
            pltpu.VMEM((SLOTS, max(width, depth), NW), BF16),
            pltpu.VMEM((tokens, width), BF16),
            pltpu.VMEM((tokens, heads), BF16),
            pltpu.VMEM((2, own, width), BF16),
            pltpu.VMEM((rows, ff), BF16),
            pltpu.VMEM((all_tiles, rows, TW), F32),
            pltpu.VMEM((all_tiles, 2, own, HW), F32),
            pltpu.VMEM((all_tiles, 2, own, TW), F32),
            pltpu.VMEM((all_tiles, rows, TW), BF16),
            pltpu.SemaphoreType.DMA((SLOTS,)),
            pltpu.SemaphoreType.DMA((4,)),
            pltpu.SemaphoreType.DMA((all_tiles,)),
            pltpu.SemaphoreType.DMA((all_tiles,)),
            pltpu.SemaphoreType.DMA((all_tiles,)),
            pltpu.SemaphoreType.DMA((all_tiles,)),
            pltpu.SemaphoreType.DMA((4,)),
            pltpu.SemaphoreType.DMA,
        ],
        compiler_params=pltpu.CompilerParams(collective_id=0, has_side_effects=True, vmem_limit_bytes=VMEM_LIMIT),
        cost_estimate=pl.CostEstimate(flops=flops, bytes_accessed=6 * width * ff * 2, transcendentals=tokens * ff),
    )(normed, x_in, attn_tok, w_o, w_gate, w_up, w_down)


def solution(mesh):
    sp_size = mesh.shape["sp"]
    tp_size = mesh.shape["tp"]
    row_spec = P(("rep", "sp"), None)
    cache_spec = P("rep", ("tp", "sp"), None)

    def layer_block(x_in, positions, norm_gain, w_q, w_k, w_v, w_o, w_gate, w_up, w_down):
        tok_local = x_in.shape[0]
        heads_tp = w_q.shape[1] // HEAD_DIM
        kv_tp = w_k.shape[1] // HEAD_DIM
        kv_repeat = sp_size // kv_tp
        normed = rms_norm(x_in, norm_gain)
        cos_tab, sin_tab = rope_tables(positions)
        q_rot = rotate(jnp.dot(normed, w_q, preferred_element_type=F32).reshape(tok_local, heads_tp, HEAD_DIM), cos_tab, sin_tab)
        k_rot = rotate(jnp.dot(normed, w_k, preferred_element_type=F32).reshape(tok_local, kv_tp, HEAD_DIM), cos_tab, sin_tab)
        v_val = jnp.dot(normed, w_v, preferred_element_type=F32).astype(BF16).reshape(tok_local, kv_tp, HEAD_DIM)
        q_send = q_rot.reshape(tok_local, sp_size, 1, HEAD_DIM)
        k_send = jnp.repeat(k_rot, kv_repeat, axis=1).reshape(tok_local, sp_size, 1, HEAD_DIM)
        v_send = jnp.repeat(v_val, kv_repeat, axis=1).reshape(tok_local, sp_size, 1, HEAD_DIM)
        send_buf = jnp.concatenate([q_send, k_send, v_send], axis=2)
        recv_buf = lax.all_to_all(send_buf, "sp", 1, 0, tiled=True)
        recv_buf = recv_buf.reshape(tok_local * sp_size, 3, HEAD_DIM)
        q_all = recv_buf[:, 0]
        k_all = recv_buf[:, 1]
        v_all = recv_buf[:, 2]
        attn_head = attention(q_all, k_all, v_all)
        attn_tok = lax.all_to_all(attn_head.reshape(sp_size * tok_local, 1, HEAD_DIM), "sp", 0, 1, tiled=True).reshape(tok_local, heads_tp * HEAD_DIM)
        y_out = ring_mlp(tp_size, normed, x_in, attn_tok, w_o, w_gate, w_up, w_down)
        return y_out, k_all[:, None, :], v_all[:, None, :]

    return jax.shard_map(
        layer_block,
        mesh=mesh,
        in_specs=(row_spec, P(("rep", "sp")), P(None), P(None, "tp"), P(None, "tp"), P(None, "tp"), P("tp", None), P(None, "tp"), P(None, "tp"), P("tp", None)),
        out_specs=(row_spec, cache_spec, cache_spec),
        check_vma=False,
    )
```
